32 devices in a mesh: wide: 8 (over z, y), narrow: 4 (over x, core).
Axes of the slice: x: 2, y: 2, z: 4, core: 2. Of those that a mesh axis runs over, the one named last changes fastest.
Arguments:
- tokens: bfloat16 [8192, 2304], P(('wide', 'narrow')), may hold values from -6 to 6
- norm_attn: bfloat16 [2304], replicated, may hold values from 0.25 to 1.75
- norm_ffn: bfloat16 [2304], replicated, may hold values from 0.25 to 1.75
- w_query: bfloat16 [2304, 2304], P('wide', 'narrow'), may hold values from -0.125 to 0.125
- w_key: bfloat16 [2304, 2304], P('wide', 'narrow'), may hold values from -0.125 to 0.125
- w_value: bfloat16 [2304, 2304], P('wide', 'narrow'), may hold values from -0.125 to 0.125
- w_out: bfloat16 [2304, 2304], P('narrow', 'wide'), may hold values from -3 to 3
- w_gate: bfloat16 [2304, 5760], P('wide', 'narrow'), may hold values from -0.125 to 0.125
- w_up: bfloat16 [2304, 5760], P('wide', 'narrow'), may hold values from -0.125 to 0.125
- w_down: bfloat16 [5760, 2304], P('narrow', 'wide'), may hold values from -0.625 to 0.625
- cotangent: bfloat16 [8192, 2304], P(('wide', 'narrow')), may hold values from -6 to 6
- lengths: int32 [2, 8], replicated, may hold values from 0 to 1024, as said below
- deal: int32 [1024], replicated, may hold values from 0 to 1023, as said below
Outputs:
- output: bfloat16 [8192, 2304], P(('wide', 'narrow'))
- grad_tokens: bfloat16 [8192, 2304], P(('wide', 'narrow'))
- grad_norm_attn: float32 [2304], replicated
- grad_norm_ffn: float32 [2304], replicated
- grad_query: float32 [2304, 2304], P('wide', 'narrow')
- grad_key: float32 [2304, 2304], P('wide', 'narrow')
- grad_value: float32 [2304, 2304], P('wide', 'narrow')
- grad_out: float32 [2304, 2304], P('narrow', 'wide')
- grad_gate: float32 [2304, 5760], P('wide', 'narrow')
- grad_up: float32 [2304, 5760], P('wide', 'narrow')
- grad_down: float32 [5760, 2304], P('narrow', 'wide')
The draws below stay inside these ranges and needn't reach their ends.
Inputs may be any that keep to these rules, and one draw needn't show every extreme that they name: Micro-batch 0: for each p, sequences 2p and 2p+1 fill stream rows 2p 512 to 2p 512 + 2 * 512 - 1 (their extents add up to 1024); sequence 0 has length 1024 and sequence 1 length 0. Micro-batch 1: sequence 0 has extent 512; for each p from 0 to 2, sequences 2p+1 and 2p+2 fill stream rows (2p+1) * 512 to (2p+3) * 512 - 1; the last sequence has extent 512; sequences 3 and 4 have lengths 1024 and 0. In both, the first sequence of each such pair has a length that is a multiple of 64. deal is a permutation of 0 .. 1023. Dealt block g and source block deal[g] lie on devices with the same index of narrow. For every two indices of wide, exactly 4 blocks of one device goes to the device with the other index of wide and the same index of narrow.
All inputs are finite; a program needn't handle non-finite values.
Results may differ from the reference program's by a relative error of at most 0.019.
Values may be sent and summed in bfloat16 or wider, within the bound.
A program may use at most 160 MiB of HBM per device.

```python
import math
import jax
import jax.numpy as jnp
from jax import lax

D = 2304
HEADS = 36
HEAD_DIM = 64
FF = 5760
TOK_DEV = 256
MB = 2
BLK = 8
UNIT = 64
RANKS = 8
LANES = 4
BLOCKS_DEV = 32
SLOT = 512
NBLK = 1024
TOKENS = 8192
N_WIDE = 8
N_NARROW = 4


def pair_lengths(key, count, unit_count, forced):
    first_key = jax.random.fold_in(key, 1)
    second_key = jax.random.fold_in(key, 2)
    split_units = jax.random.randint(first_key, (count,), 0, unit_count + 1)
    split_units = split_units.at[forced].set(unit_count)
    padding = jax.random.randint(second_key, (count,), 0, UNIT)
    first_len = split_units * UNIT
    second_extent = (unit_count - split_units) * UNIT
    second_len = jnp.maximum(second_extent - padding, 0)
    return jnp.stack([first_len, second_len], axis=1).reshape(-1)


def draw_lengths(key, part):
    pair_count = RANKS // 2
    unit_count = 2 * SLOT // UNIT
    row_first = pair_lengths(jax.random.fold_in(key, 11), pair_count, unit_count, 0)
    inner = pair_lengths(jax.random.fold_in(key, 12), pair_count - 1, unit_count, pair_count // 2 - 1)
    edge_pad = jax.random.randint(jax.random.fold_in(key, 13), (2,), 0, UNIT)
    edges = SLOT - edge_pad
    row_second = jnp.concatenate([edges[0:1], inner, edges[1:2]])
    return jnp.stack([row_first, row_second], axis=0).astype(jnp.int32)


def draw_deal(key, part):
    shift_key = jax.random.fold_in(key, 21)
    order_key = jax.random.fold_in(key, 22)
    offset = jax.random.randint(shift_key, (), 0, RANKS)
    keys_all = jax.random.split(order_key, RANKS * LANES)
    orders = jax.vmap(lambda one_key: jax.random.permutation(one_key, BLOCKS_DEV))(keys_all)
    orders = orders.reshape(RANKS, LANES, BLOCKS_DEV)
    dest_rank = jnp.arange(RANKS, dtype=jnp.int32)[:, None, None]
    lane_index = jnp.arange(LANES, dtype=jnp.int32)[None, :, None]
    slot_index = jnp.arange(BLOCKS_DEV, dtype=jnp.int32)[None, None, :]
    source_rank = (dest_rank + offset + slot_index) % RANKS
    local_index = orders[source_rank, lane_index, slot_index]
    dealt = (source_rank * LANES + lane_index) * BLOCKS_DEV + local_index
    return dealt.reshape(-1).astype(jnp.int32)


def shard_levels(key, dims, cuts, smallest, largest):
    level = 1.0
    for dim, blocks in cuts:
        heights = jax.random.uniform(jax.random.fold_in(jax.random.fold_in(key, 6), dim), (blocks,), jnp.float32, smallest / len(cuts), largest / len(cuts))
        level = level * jnp.repeat(jnp.exp(heights), dims[dim] // blocks).reshape((-1,) + (1,) * (len(dims) - 1 - dim))
    return level


def gaussian(rng, dims, width, limit, cuts=(), kind=jnp.bfloat16):
    values = width * jax.random.normal(rng, dims, jnp.float32)
    if cuts:
        values = values * shard_levels(rng, dims, cuts, -0.22, 0.18)
    return jnp.clip(values, -limit, limit).astype(kind)


def setup_inputs(seed: int = 0) -> dict:
    key_list = jax.random.split(jax.random.key(seed), 14)
    tokens = gaussian(key_list[0], (TOKENS, D), 1.0, 6.0, ((0, 32),))
    norm_attn = jnp.clip(1.0 + 0.15 * jax.random.normal(key_list[1], (D,), jnp.float32), 0.25, 1.75).astype(jnp.bfloat16)
    norm_ffn = jnp.clip(1.0 + 0.15 * jax.random.normal(key_list[2], (D,), jnp.float32), 0.25, 1.75).astype(jnp.bfloat16)
    w_query = gaussian(key_list[3], (D, D), D ** -0.5, 0.125, ((0, 8), (1, 4)))
    w_key = gaussian(key_list[4], (D, D), D ** -0.5, 0.125, ((0, 8), (1, 4)))
    w_value = gaussian(key_list[5], (D, D), D ** -0.5, 0.125, ((0, 8), (1, 4)))
    w_out = gaussian(key_list[6], (D, D), 0.5, 3.0, ((0, 4), (1, 8)))
    w_gate = gaussian(key_list[7], (D, FF), D ** -0.5, 0.125, ((0, 8), (1, 4)))
    w_up = gaussian(key_list[8], (D, FF), D ** -0.5, 0.125, ((0, 8), (1, 4)))
    w_down = gaussian(key_list[9], (FF, D), (FF // 64) ** -0.5, 0.625, ((0, 4), (1, 8)))
    cotangent = gaussian(key_list[10], (TOKENS, D), 1.0, 6.0, ((0, 32),))
    lengths = draw_lengths(jax.random.fold_in(key_list[13], 71), 0)
    deal = draw_deal(jax.random.fold_in(key_list[13], 71), 0)
    return dict(tokens=tokens, norm_attn=norm_attn, norm_ffn=norm_ffn, w_query=w_query, w_key=w_key, w_value=w_value, w_out=w_out, w_gate=w_gate, w_up=w_up, w_down=w_down, cotangent=cotangent, lengths=lengths, deal=deal)


@jax.custom_vjp
def low(v):
    return lax.optimization_barrier(v.astype(jnp.bfloat16)).astype(jnp.float32)

@jax.custom_vjp
def low_back(v):
    return v

def low_keep(v):
    return (low(v), None)

def low_pass(kept, grad):
    return (grad,)

def back_keep(v):
    return (v, None)

def back_low(kept, grad):
    return (low(grad),)
low.defvjp(low_keep, low_pass)
low_back.defvjp(back_keep, back_low)
BRANCH = 1.4 / math.sqrt(40.0)
EPSILON = 1e-05
NEGATIVE = -1e+30
PRECISE = lax.Precision.HIGHEST

def rotate(field_in, position, direction):
    head_count = field_in.shape[1] // HEAD_DIM
    half_dim = HEAD_DIM // 2
    counter = jnp.arange(half_dim, dtype=jnp.float32)
    frequency = jnp.exp(counter * (-2.0 * math.log(10000.0) / HEAD_DIM))
    phase_angle = position.astype(jnp.float32)[:, None] * frequency[None, :]
    cosine = jnp.concatenate([jnp.cos(phase_angle), jnp.cos(phase_angle)], axis=1)[:, None, :]
    sine_table = jnp.concatenate([jnp.sin(phase_angle), jnp.sin(phase_angle)], axis=1)[:, None, :]
    shaped = field_in.reshape(field_in.shape[0], head_count, HEAD_DIM)
    turned = jnp.concatenate([-shaped[:, :, half_dim:], shaped[:, :, :half_dim]], axis=2)
    return (shaped * cosine + direction * turned * sine_table).reshape(field_in.shape)

def matmul(left, right):
    return jnp.dot(left, right, precision=PRECISE)

def to_streams(flat_rows, deal):
    pieces = flat_rows.reshape(NBLK, BLK, D)[deal]
    shaped = pieces.reshape(N_WIDE, N_NARROW, MB, TOK_DEV // MB, D)
    return shaped.transpose(2, 0, 1, 3, 4).reshape(MB, N_WIDE * SLOT, D)

def from_streams(streams, deal):
    shaped = streams.reshape(MB, N_WIDE, N_NARROW, TOK_DEV // MB, D).transpose(1, 2, 0, 3, 4)
    pieces = shaped.reshape(NBLK, BLK, D)
    return jnp.zeros_like(pieces).at[deal].set(pieces).reshape(TOKENS, D)

def stream_layout(lengths):
    extent = (lengths + UNIT - 1) // UNIT * UNIT
    begin = jnp.cumsum(extent, axis=1) - extent
    places = jnp.arange(N_WIDE * SLOT, dtype=jnp.int32)
    ending = begin + lengths
    inside = (places[None, :, None] >= begin[:, None, :]) & (places[None, :, None] < ending[:, None, :])
    number = jnp.arange(N_WIDE, dtype=jnp.int32) + 1
    segment = (lax.optimization_barrier(jnp.sum(jnp.where(inside, number[None, None, :], 0), axis=2)) - 1).astype(jnp.int32)
    position = (places[None, :] - lax.optimization_barrier(jnp.sum(jnp.where(inside, begin[:, None, :], 0), axis=2))).astype(jnp.int32)
    return (segment, position)

def rank_attention(queries, keys, values, segment):
    query_three = queries.reshape(SLOT, HEADS, HEAD_DIM)
    key_three = keys.reshape(2 * SLOT, HEADS, HEAD_DIM)
    value_three = values.reshape(2 * SLOT, HEADS, HEAD_DIM)
    scores = jnp.einsum('qhd,khd->hqk', query_three, key_three, precision=PRECISE)
    scores = low_back(scores * (1.0 / math.sqrt(HEAD_DIM)))
    query_index = SLOT + jnp.arange(SLOT, dtype=jnp.int32)
    key_index = jnp.arange(2 * SLOT, dtype=jnp.int32)
    query_segment = segment[SLOT:]
    allowed = (query_segment[:, None] == segment[None, :]) & (query_segment[:, None] >= 0) & (key_index[None, :] <= query_index[:, None]) | (key_index[None, :] == query_index[:, None])
    scores = jnp.where(allowed[None, :, :], scores, NEGATIVE)
    top_score = lax.optimization_barrier(jnp.max(scores, axis=2, keepdims=True))
    weights_exp = jnp.exp(scores - top_score)
    probs = weights_exp / lax.optimization_barrier(jnp.sum(weights_exp, axis=2, keepdims=True))
    mixed = jnp.einsum('hqk,khd->qhd', low(probs), value_three, precision=PRECISE)
    return mixed.reshape(SLOT, HEADS * HEAD_DIM)

def step_rank(carry, parts):
    return (carry, jax.checkpoint(rank_attention)(*parts))

def with_previous(field_in, fill):
    shaped = field_in.reshape((N_WIDE, SLOT) + field_in.shape[1:])
    first = jnp.full((1, SLOT) + field_in.shape[1:], fill, field_in.dtype)
    earlier = jnp.concatenate([first, shaped[:-1]], axis=0)
    return jnp.concatenate([earlier, shaped], axis=1)

def layer(streams, gain_attn, gain_ffn, wq, wk, wv, wo, wg, wu, wd, validity, segment, position):
    results = []
    for micro in range(MB):
        resid = streams[micro] * validity[micro][:, None]
        rate_attn = lax.rsqrt(lax.optimization_barrier(jnp.mean(resid * resid, axis=1, keepdims=True)) + EPSILON)
        attn_in = low(resid * rate_attn * gain_attn[None, :])
        queries = low(rotate(low_back(matmul(attn_in, wq)), position[micro], 1.0))
        keys = low(rotate(low_back(matmul(attn_in, wk)), position[micro], 1.0))
        values = low(low_back(matmul(attn_in, wv)))
        carry_out, mixed = lax.scan(step_rank, jnp.zeros((), jnp.float32), (queries.reshape(N_WIDE, SLOT, D), with_previous(keys, 0.0), with_previous(values, 0.0), with_previous(segment[micro], -1)))
        attn_out = low(low_back(mixed.reshape(N_WIDE * SLOT, D)))
        branch_attn = low_back(matmul(attn_out, wo))
        middle = resid + BRANCH * branch_attn
        rate_ffn = lax.rsqrt(lax.optimization_barrier(jnp.mean(middle * middle, axis=1, keepdims=True)) + EPSILON)
        ffn_in = low(middle * rate_ffn * gain_ffn[None, :])
        gate = low_back(matmul(ffn_in, wg))
        upward = low_back(matmul(ffn_in, wu))
        hidden = low(jax.nn.silu(gate) * upward)
        branch_ffn = low_back(matmul(hidden, wd))
        results.append(middle + BRANCH * branch_ffn)
    return jnp.stack(results)

def reference(tokens, norm_attn, norm_ffn, w_query, w_key, w_value, w_out, w_gate, w_up, w_down, cotangent, lengths, deal):
    segment, position = stream_layout(lengths)
    validity = (segment >= 0).astype(jnp.float32)
    streams = to_streams(tokens, deal).astype(jnp.float32)
    cot_streams = to_streams(cotangent, deal).astype(jnp.float32)
    params = tuple((weight_arg.astype(jnp.float32) for weight_arg in (norm_attn, norm_ffn, w_query, w_key, w_value, w_out, w_gate, w_up, w_down)))

    def forward(streams_in, *weights_in):
        return layer(streams_in, *weights_in, validity, segment, position)
    result, pullback = jax.vjp(forward, streams, *params)
    grads = pullback(cot_streams)
    output = from_streams(result.astype(jnp.bfloat16), deal)
    grad_tokens = from_streams(grads[0].astype(jnp.bfloat16), deal)
    return (output, grad_tokens, grads[1], grads[2], grads[3], grads[4], grads[5], grads[6], grads[7], grads[8], grads[9])
```

```python
import functools
import math

import jax
import jax.numpy as jnp
from jax import lax
from jax.experimental import pallas as pl
from jax.experimental.layout import Layout, with_layout_constraint
from jax.experimental.pallas import tpu as pltpu
from jax.sharding import PartitionSpec as P

HEAD_DIM = 64
MB = 2
BLK = 8
UNIT = 64

BRANCH = 1.4 / math.sqrt(40.0)
EPSILON = 1e-05
NEGATIVE = -1e30
SCALE = 1.0 / math.sqrt(HEAD_DIM)
LONGEST_RING = 8


def tie(*values):
    return lax.optimization_barrier(values)


def ring_tables(count):
    order = list(range(0, count, 2)) + list(range(count - 1, 0, -2))
    ahead = [(order[i], order[(i + 1) % count]) for i in range(count)]
    behind = [(b, a) for a, b in ahead]
    return ahead, behind


def ring_place(index, count):
    odd = index % 2
    return (1 - odd) * (index // 2) + odd * (count - 1 - index // 2)


def ring_index(place, count):
    place = (place + 2 * count) % count
    late = place // (count // 2)
    return (1 - late) * (2 * place) + late * (2 * (count - 1 - place) + 1)


class Ring:
    def __init__(self):
        self.count = lax.axis_size("wide")
        self.rank = lax.axis_index("wide")
        self.place = ring_place(self.rank, self.count)
        self.ahead, self.behind = ring_tables(self.count)

    def gather(self, shard, after=None, between=None):
        kinds, rows, columns = shard.shape
        if self.count > LONGEST_RING:
            for make in (between or {}).values():
                make()
            return lax.all_gather(shard, "wide", axis=1, tiled=True), None
        half = rows // 2
        top, bottom = shard[:, :half], shard[:, half:]
        if after is not None:
            top, bottom, _ = tie(top, bottom, after[-2])
        full = jnp.zeros((kinds, self.count * rows, columns), shard.dtype)
        full = lax.dynamic_update_slice(full, shard, (0, self.rank * rows, 0))
        marks = []
        for step in range(1, self.count):
            if between is not None and step in between:
                top, bottom, _ = tie(top, bottom, between[step]())
            top = lax.ppermute(top, "wide", self.ahead)
            bottom = lax.ppermute(bottom, "wide", self.behind)
            marks.append((top, bottom))
            full = lax.dynamic_update_slice(
                full, top, (0, ring_index(self.place - step, self.count) * rows, 0)
            )
            full = lax.dynamic_update_slice(
                full, bottom, (0, ring_index(self.place + step, self.count) * rows + half, 0)
            )
        return full, marks

    def scatter(self, wholes):
        if self.count > LONGEST_RING:
            parts = [lax.psum_scatter(w, "wide", scatter_dimension=0, tiled=True) for w in wholes]
            return jnp.stack(parts).astype(jnp.float32)
        wholes = [with_layout_constraint(whole, Layout(major_to_minor=(0, 1))) for whole in wholes]
        wholes = tie(*wholes)
        rows = wholes[0].shape[0] // self.count
        half = rows // 2

        def own(place, low):
            start = ring_index(place, self.count) * rows + low
            return jnp.stack(
                [lax.dynamic_slice_in_dim(whole, start, half) for whole in wholes]
            )

        top = own(self.place - 1, 0)
        bottom = own(self.place + 1, half)
        for step in range(1, self.count):
            top = lax.ppermute(top, "wide", self.ahead)
            bottom = lax.ppermute(bottom, "wide", self.behind)
            top = top.astype(jnp.float32) + own(self.place - 1 - step, 0).astype(jnp.float32)
            bottom = bottom.astype(jnp.float32) + own(self.place + 1 + step, half).astype(
                jnp.float32
            )
            if step < self.count - 1:
                top, bottom = top.astype(jnp.bfloat16), bottom.astype(jnp.bfloat16)
        return jnp.concatenate([top, bottom], axis=1)


def swap(block, bit):
    route = [(i, i ^ bit) for i in range(lax.axis_size("narrow"))]
    return lax.ppermute(block, "narrow", route)


def narrow_gather(block):
    far = swap(block, 2)
    near = swap(block, 1)
    cross = swap(far, 1)
    return jnp.stack([block, near, far, cross], axis=1).reshape(-1, block.shape[2])


def narrow_scatter(parts):
    got = swap(jnp.stack([parts[:, 1], parts[:, 3]]), 1).astype(jnp.float32)
    mine = parts[:, 0].astype(jnp.float32) + got[0]
    theirs = (parts[:, 2].astype(jnp.float32) + got[1]).astype(jnp.bfloat16)
    return (mine + swap(theirs, 2).astype(jnp.float32)).reshape(-1, parts.shape[3])


def total_over_all(value):
    for axis in ("narrow", "wide"):
        count = lax.axis_size(axis)
        bit = 1
        while bit < count:
            value = value + lax.ppermute(value, axis, [(i, i ^ bit) for i in range(count)])
            bit *= 2
    return value


def rotation_tables(position):
    lane = jnp.arange(2 * HEAD_DIM, dtype=jnp.int32)
    counter = (lane % (HEAD_DIM // 2)).astype(jnp.float32)
    frequency = jnp.exp(counter * (-2.0 * math.log(10000.0) / HEAD_DIM))
    phase_angle = position.astype(jnp.float32)[:, None] * frequency[None, :]
    sign = jnp.where(lane % HEAD_DIM < HEAD_DIM // 2, -1.0, 1.0)
    return jnp.cos(phase_angle), jnp.sin(phase_angle) * sign[None, :]


def turned(pair):
    lane = lax.broadcasted_iota(jnp.int32, pair.shape, 1)
    return jnp.where(
        lane % HEAD_DIM < HEAD_DIM // 2,
        pltpu.roll(pair, 2 * HEAD_DIM - HEAD_DIM // 2, 1),
        pltpu.roll(pair, HEAD_DIM // 2, 1),
    )


def project_kernel(x_ref, w_ref, cos_ref, sin_ref, out_ref, scratch):
    columns = out_ref.shape[2]
    field = jnp.dot(x_ref[...], w_ref[0], preferred_element_type=jnp.float32)

    @pl.when(pl.program_id(0) == 2)
    def _():
        out_ref[0] = field.astype(jnp.bfloat16)

    @pl.when(pl.program_id(0) < 2)
    def _():
        scratch[:, :columns] = field
        for low in range(0, columns, 128):
            pair = scratch[:, low : low + 128]
            value = (pair * cos_ref[...] + turned(pair) * sin_ref[...]).astype(jnp.bfloat16)
            high = min(columns, low + 128)
            out_ref[0, :, low:high] = value[:, : high - low]


def project(rows, stack, tables):
    count, width = rows.shape
    columns = stack.shape[2]
    padded = (columns + 127) // 128 * 128
    whole = lambda i: (0, 0)
    return pl.pallas_call(
        project_kernel,
        out_shape=jax.ShapeDtypeStruct((3, count, columns), jnp.bfloat16),
        grid=(3,),
        in_specs=[
            pl.BlockSpec((count, width), whole),
            pl.BlockSpec((1, width, columns), lambda i: (i, 0, 0)),
            pl.BlockSpec((count, 128), whole),
            pl.BlockSpec((count, 128), whole),
        ],
        out_specs=pl.BlockSpec((1, count, columns), lambda i: (i, 0, 0)),
        scratch_shapes=[pltpu.VMEM((count, padded), jnp.float32)],
        cost_estimate=pl.CostEstimate(
            flops=6 * count * width * columns,
            bytes_accessed=2 * (count * width + 3 * width * columns + 3 * count * columns),
            transcendentals=0,
        ),
        compiler_params=pltpu.CompilerParams(vmem_limit_bytes=48 * 1024 * 1024),
        name="project",
    )(rows, stack, *tables)


def dot_t(left, right):
    return lax.dot_general(
        left, right, (((1,), (1,)), ((), ())), preferred_element_type=jnp.float32
    )


def dot_n(left, right):
    return jnp.dot(left, right, preferred_element_type=jnp.float32)


def attend_kernel(columns, qkv_ref, prev_ref, bias_one, bias_two, out_ref, prob_one, prob_two):
    rows = prev_ref.shape[1]
    lane = lax.broadcasted_iota(jnp.int32, (rows, 128), 1)
    real = columns - 128 * pl.program_id(0)

    def clean(value):
        return jnp.where(lane < real, value, jnp.zeros_like(value))

    q_one, q_two = clean(qkv_ref[0, :rows]) * SCALE, clean(qkv_ref[0, rows:]) * SCALE
    q_one, q_two = q_one.astype(jnp.bfloat16), q_two.astype(jnp.bfloat16)
    k_one = jnp.concatenate([clean(prev_ref[0]), clean(qkv_ref[1, :rows])], axis=0)
    v_one = jnp.concatenate([clean(prev_ref[1]), clean(qkv_ref[2, :rows])], axis=0)
    k_two, v_two = clean(qkv_ref[1, rows:]), clean(qkv_ref[2, rows:])
    for part, (query, keys, values, bias, prob) in enumerate(
        ((q_one, k_one, v_one, bias_one, prob_one), (q_two, k_two, v_two, bias_two, prob_two))
    ):
        values_t = values.T
        mixed = []
        for head in range(2):
            mine = lane // HEAD_DIM == head
            score = dot_t(keys, jnp.where(mine, query, jnp.zeros_like(query))) + bias[...]
            raised = jnp.exp(score - jnp.max(score, axis=0, keepdims=True))
            chance = (raised * (1.0 / jnp.sum(raised, axis=0, keepdims=True))).astype(jnp.bfloat16)
            prob[head] = chance
            mixed.append(dot_n(values_t[head * HEAD_DIM : (head + 1) * HEAD_DIM], chance))
        out_ref[part * rows : (part + 1) * rows] = (
            jnp.concatenate(mixed, axis=0).T.astype(jnp.bfloat16)
        )


def attend(qkv, prev, bias_one, bias_two):
    _, count, columns = qkv.shape
    rows = count // 2
    steps = (columns + 127) // 128
    whole = lambda j: (0, 0)
    return pl.pallas_call(
        functools.partial(attend_kernel, columns),
        out_shape=[
            jax.ShapeDtypeStruct((count, columns), jnp.bfloat16),
            jax.ShapeDtypeStruct((columns // HEAD_DIM, 2 * rows, rows), jnp.bfloat16),
            jax.ShapeDtypeStruct((columns // HEAD_DIM, rows, rows), jnp.bfloat16),
        ],
        grid=(steps,),
        in_specs=[
            pl.BlockSpec((3, count, 128), lambda j: (0, 0, j)),
            pl.BlockSpec((2, rows, 128), lambda j: (0, 0, j)),
            pl.BlockSpec((2 * rows, rows), whole),
            pl.BlockSpec((rows, rows), whole),
        ],
        out_specs=[
            pl.BlockSpec((count, 128), lambda j: (0, j)),
            pl.BlockSpec((2, 2 * rows, rows), lambda j: (j, 0, 0)),
            pl.BlockSpec((2, rows, rows), lambda j: (j, 0, 0)),
        ],
        cost_estimate=pl.CostEstimate(
            flops=12 * rows * rows * columns,
            bytes_accessed=2 * (4 * count * columns + 3 * 10 * rows * rows),
            transcendentals=3 * 9 * rows * rows,
        ),
        compiler_params=pltpu.CompilerParams(vmem_limit_bytes=48 * 1024 * 1024),
        name="attend",
    )(qkv, prev, bias_one, bias_two)


def attend_back_kernel(
    columns, qkv_ref, prev_ref, ob_ref, dob_ref, prob_one, prob_two, cos_ref, sin_ref,
    cos_prev, sin_prev, dq_ref, one_ref, two_ref, prev_out
):
    rows = prev_ref.shape[1]
    lane = lax.broadcasted_iota(jnp.int32, (rows, 128), 1)
    real = columns - 128 * pl.program_id(0)

    def clean(value):
        return jnp.where(lane < real, value, jnp.zeros_like(value))

    def unrotate(value, cosine, sine):
        return value * cosine - turned(value) * sine

    k_prev, k_first = clean(prev_ref[0]), clean(qkv_ref[1, :rows])
    v_prev, v_first = clean(prev_ref[1]), clean(qkv_ref[2, :rows])
    parts = (
        (
            jnp.concatenate([k_prev, k_first], axis=0),
            jnp.concatenate([v_prev, v_first], axis=0),
            prob_one,
        ),
        (clean(qkv_ref[1, rows:]), clean(qkv_ref[2, rows:]), prob_two),
    )
    for part, (keys, values, prob) in enumerate(parts):
        here = slice(part * rows, (part + 1) * rows)
        cosine, sine = cos_ref[here], sin_ref[here]
        query = (clean(qkv_ref[0, here]) * SCALE).astype(jnp.bfloat16)
        dob, ob = clean(dob_ref[here]), clean(ob_ref[here])
        product = (dob.astype(jnp.float32) * ob.astype(jnp.float32)).T
        keys_t = keys.T
        dq, dk, dv = [], [], []
        for head in range(2):
            mine = lane // HEAD_DIM == head
            span = slice(head * HEAD_DIM, (head + 1) * HEAD_DIM)
            chance = prob[head]
            dprob = dot_t(values, jnp.where(mine, dob, jnp.zeros_like(dob)))
            delta = jnp.sum(product[span], axis=0, keepdims=True)
            dscore = (chance.astype(jnp.float32) * (dprob - delta)).astype(jnp.bfloat16)
            dq.append(dot_n(keys_t[span], dscore))
            dk.append(dot_n(dscore, query))
            dv.append(dot_n(chance, dob))
        dq = jnp.concatenate(dq, axis=0).T * SCALE
        dq_ref[here] = unrotate(dq, cosine, sine).astype(jnp.bfloat16)
        wide_lane = lax.broadcasted_iota(jnp.int32, dk[0].shape, 1)
        dk = jnp.where(wide_lane < HEAD_DIM, dk[0], dk[1])
        dv = jnp.where(wide_lane < HEAD_DIM, dv[0], dv[1])
        if part == 0:
            prev_out[0] = unrotate(dk[:rows], cos_prev[...], sin_prev[...]).astype(jnp.bfloat16)
            prev_out[1] = dv[:rows].astype(jnp.bfloat16)
            one_ref[0] = unrotate(dk[rows:], cosine, sine).astype(jnp.bfloat16)
            one_ref[1] = dv[rows:].astype(jnp.bfloat16)
        else:
            two_ref[0] = unrotate(dk, cosine, sine)
            two_ref[1] = dv


def attend_back(qkv, prev, mixed, grad_mixed, prob_one, prob_two, tables, tables_prev):
    _, count, columns = qkv.shape
    rows = count // 2
    steps = (columns + 127) // 128
    whole = lambda j: (0, 0)
    pair = lambda j: (0, j)
    layered = lambda j: (0, 0, j)
    return pl.pallas_call(
        functools.partial(attend_back_kernel, columns),
        out_shape=[
            jax.ShapeDtypeStruct((count, columns), jnp.bfloat16),
            jax.ShapeDtypeStruct((2, rows, columns), jnp.bfloat16),
            jax.ShapeDtypeStruct((2, rows, columns), jnp.float32),
            jax.ShapeDtypeStruct((2, rows, columns), jnp.bfloat16),
        ],
        grid=(steps,),
        in_specs=[
            pl.BlockSpec((3, count, 128), layered),
            pl.BlockSpec((2, rows, 128), layered),
            pl.BlockSpec((count, 128), pair),
            pl.BlockSpec((count, 128), pair),
            pl.BlockSpec((2, 2 * rows, rows), lambda j: (j, 0, 0)),
            pl.BlockSpec((2, rows, rows), lambda j: (j, 0, 0)),
            pl.BlockSpec((count, 128), whole),
            pl.BlockSpec((count, 128), whole),
            pl.BlockSpec((rows, 128), whole),
            pl.BlockSpec((rows, 128), whole),
        ],
        out_specs=[
            pl.BlockSpec((count, 128), pair),
            pl.BlockSpec((2, rows, 128), layered),
            pl.BlockSpec((2, rows, 128), layered),
            pl.BlockSpec((2, rows, 128), layered),
        ],
        cost_estimate=pl.CostEstimate(
            flops=24 * rows * rows * columns,
            bytes_accessed=2 * (10 * count * columns + 3 * 10 * rows * rows),
            transcendentals=0,
        ),
        compiler_params=pltpu.CompilerParams(vmem_limit_bytes=56 * 1024 * 1024),
        name="attend_back",
    )(qkv, prev, mixed, grad_mixed, prob_one, prob_two, *tables, *tables_prev)


def transpose_kernel(out_ref, down_ref, out_t, down_t):
    out_t[...] = out_ref[...].T
    down_t[...] = down_ref[...].T


def transposed(w_out, w_down):
    return pl.pallas_call(
        transpose_kernel,
        out_shape=[
            jax.ShapeDtypeStruct(w_out.shape[::-1], w_out.dtype),
            jax.ShapeDtypeStruct(w_down.shape[::-1], w_down.dtype),
        ],
        name="transposed",
    )(w_out, w_down)


def contract(left, right, left_dim, right_dim):
    return lax.dot_general(
        left, right, (((left_dim,), (right_dim,)), ((), ())), preferred_element_type=jnp.float32
    )


def norm_rate(resid):
    return lax.rsqrt(jnp.mean(resid * resid, axis=1, keepdims=True) + EPSILON)


def norm_backward(grad_in, resid, rate, gain):
    scaled_grad = grad_in * gain[None, :]
    return rate * scaled_grad - resid * rate**3 * jnp.mean(
        scaled_grad * resid, axis=1, keepdims=True
    )


def invert_order(placing):
    counter = jnp.arange(placing.shape[0], dtype=jnp.int32)
    return jnp.sum(jnp.where(placing[None, :] == counter[:, None], counter[None, :], 0), axis=1)


def deal_routes(deal, my_rank, my_lane, rank_count, lane_count, block_count, turn):
    per_pair = block_count // rank_count
    base_block = (my_rank * lane_count + my_lane) * block_count
    counter = jnp.arange(block_count, dtype=jnp.int32)
    every_block = jnp.arange(deal.shape[0], dtype=jnp.int32)
    owned = base_block + counter
    target = jnp.sum(jnp.where(deal[None, :] == owned[:, None], every_block[None, :], 0), axis=1)
    target_rank = target // (lane_count * block_count)
    target_slot = target % block_count
    earlier = (target_rank[None, :] == target_rank[:, None]) & (
        target_slot[None, :] < target_slot[:, None]
    )
    shift = (target_rank - my_rank + rank_count) % rank_count
    send_place = shift * per_pair + jnp.sum(earlier.astype(jnp.int32), axis=1)
    mine = lax.dynamic_slice_in_dim(deal, base_block, block_count)
    source_rank = mine // (lane_count * block_count)
    before = (source_rank[None, :] == source_rank[:, None]) & (counter[None, :] < counter[:, None])
    back_shift = (my_rank - source_rank + rank_count) % rank_count
    recv_place = back_shift * per_pair + jnp.sum(before.astype(jnp.int32), axis=1)
    half = block_count // MB
    recv_place = jnp.where(
        turn == 1, jnp.concatenate([recv_place[half:], recv_place[:half]]), recv_place
    )
    return send_place, recv_place


def exchange(packed, direction):
    count = lax.axis_size("wide")
    if count > LONGEST_RING:
        index = (lax.axis_index("wide") + direction * jnp.arange(count)) % count
        placed = jnp.zeros_like(packed).at[index].set(packed)
        got = lax.all_to_all(placed, "wide", split_axis=0, concat_axis=0, tiled=True)
        return got[(lax.axis_index("wide") - direction * jnp.arange(count)) % count]
    groups = [packed[0]]
    for k in range(1, count):
        route = [(i, (i + direction * k) % count) for i in range(count)]
        groups.append(lax.ppermute(packed[k], "wide", route))
    return jnp.stack(groups)


def layout_of(length_row, places):
    extent = (length_row + UNIT - 1) // UNIT * UNIT
    begin = jnp.cumsum(extent) - extent
    ending = begin + length_row
    inside = (places[:, None] >= begin[None, :]) & (places[:, None] < ending[None, :])
    number = jnp.arange(length_row.shape[0], dtype=jnp.int32) + 1
    segment = jnp.sum(jnp.where(inside, number[None, :], 0), axis=1) - 1
    position = places - jnp.sum(jnp.where(inside, begin[None, :], 0), axis=1)
    return segment, position


def allowed_bias(key_segment, key_place, query_segment, query_place):
    same = (query_segment[None, :] == key_segment[:, None]) & (query_segment[None, :] >= 0)
    allowed = same & (key_place[:, None] <= query_place[None, :]) | (
        key_place[:, None] == query_place[None, :]
    )
    return jnp.where(allowed, 0.0, NEGATIVE)


def body(
    tokens,
    norm_attn,
    norm_ffn,
    w_query,
    w_key,
    w_value,
    w_out,
    w_gate,
    w_up,
    w_down,
    cotangent,
    lengths,
    deal,
):
    rank_count = lax.axis_size("wide")
    lane_count = lax.axis_size("narrow")
    my_rank = lax.axis_index("wide")
    my_lane = lax.axis_index("narrow")
    row_count, width = tokens.shape
    block_count = row_count // BLK
    per_pair = block_count // rank_count
    micro_rows = row_count // MB
    slot_rows = lane_count * micro_rows
    ring = Ring()

    reaching = 1 - my_rank % 2
    send_place, recv_place = deal_routes(
        deal, my_rank, my_lane, rank_count, lane_count, block_count, reaching
    )
    send_order = invert_order(send_place)
    back_order = invert_order(recv_place)

    def packed(flat_rows, order):
        return flat_rows.reshape(block_count, BLK, width)[order].reshape(
            rank_count, per_pair * BLK, width
        )

    def unpacked(groups, placing):
        return groups.reshape(block_count, BLK, width)[placing].reshape(row_count, width)

    both = exchange(
        jnp.stack([packed(tokens, send_order), packed(cotangent, send_order)], axis=1), 1
    )
    x_rows = unpacked(both[:, 0], recv_place)
    cot_rows = unpacked(both[:, 1], recv_place)

    wo_t, wd_t = transposed(w_out, w_down)
    stack_attn = jnp.stack([w_query, w_key, w_value, wo_t])
    full_attn, marks = ring.gather(stack_attn)
    wg_full, marks = ring.gather(w_gate[None], after=marks)
    wg_full = wg_full[0]
    wq_full, wk_full, wv_full, wo_full = (full_attn[i] for i in range(4))

    gain_attn = norm_attn.astype(jnp.float32)
    gain_ffn = norm_ffn.astype(jnp.float32)

    lane_rows = jnp.arange(micro_rows, dtype=jnp.int32)
    lanes_near = jnp.bitwise_xor(my_lane, jnp.arange(lane_count, dtype=jnp.int32))
    places = (
        my_rank * slot_rows + lanes_near[:, None] * micro_rows + lane_rows[None, :]
    ).reshape(-1)
    lengths_one = lax.dynamic_index_in_dim(lengths, reaching, 0, keepdims=False)
    lengths_two = lax.dynamic_index_in_dim(lengths, 1 - reaching, 0, keepdims=False)
    key_places = jnp.concatenate([places - slot_rows, places])
    segment_one, position_one = layout_of(lengths_one, key_places)
    segment_two, position_two = layout_of(lengths_two, places)
    bias_one = allowed_bias(segment_one, key_places, segment_one[slot_rows:], places)
    bias_two = allowed_bias(segment_two, places, segment_two, places)
    tables = rotation_tables(jnp.concatenate([position_one[slot_rows:], position_two]))
    tables_prev = rotation_tables(position_one[:slot_rows])
    valid = jnp.concatenate(
        [segment_one[slot_rows : slot_rows + micro_rows], segment_two[:micro_rows]]
    )
    validity = (valid >= 0).astype(jnp.float32)[:, None]

    def gathered(block):
        return narrow_gather(block.reshape(MB, micro_rows, width))

    def summed(rows):
        return narrow_scatter(rows.astype(jnp.bfloat16).reshape(MB, lane_count, micro_rows, width))

    resid = x_rows.astype(jnp.float32) * validity
    rate_attn = norm_rate(resid)
    attn_rows = gathered((resid * rate_attn * gain_attn[None, :]).astype(jnp.bfloat16))
    qkv = project(attn_rows, full_attn, tables)
    route = [(i, i + 1) for i in range(rank_count - 1)]
    prev = lax.ppermute(qkv[1:, slot_rows:], "wide", route)
    attn_out, prob_one, prob_two = attend(qkv, prev, bias_one, bias_two)
    middle = resid + BRANCH * summed(contract(attn_out, wo_full, 1, 1))
    rate_ffn = norm_rate(middle)
    ffn_rows = gathered((middle * rate_ffn * gain_ffn[None, :]).astype(jnp.bfloat16))
    cot_branch = gathered((BRANCH * cot_rows.astype(jnp.float32)).astype(jnp.bfloat16))
    made = {}

    def make_gate():
        made["gate"] = contract(ffn_rows, wg_full, 1, 0).astype(jnp.bfloat16)
        return made["gate"]

    def make_hidden():
        gate, upward = tie(
            made["gate"], contract(ffn_rows, wu_full, 1, 0).astype(jnp.bfloat16)
        )
        gate, upward = gate.astype(jnp.float32), upward.astype(jnp.float32)
        sigma = jax.nn.sigmoid(gate)
        made["hidden"] = (gate * sigma * upward).astype(jnp.bfloat16)
        made["parts"] = gate, upward, sigma
        return made["hidden"]

    def make_grad_down():
        made["grad_wd"] = contract(cot_branch, made["hidden"], 0, 0).astype(jnp.bfloat16)
        return made["grad_wd"]

    wu_full, marks = ring.gather(w_up[None], after=marks, between={4: make_gate})
    wu_full = wu_full[0]
    full_down, marks = ring.gather(
        wd_t[None], after=marks, between={3: make_hidden, 5: make_grad_down}
    )
    full_down = full_down[0]
    hidden, (gate, upward, sigma) = made["hidden"], made["parts"]
    sum_down = ring.scatter([made["grad_wd"]])
    grad_hidden = contract(cot_branch, full_down, 1, 0)
    grad_gate = (grad_hidden * upward * sigma * (1.0 + gate * (1.0 - sigma))).astype(jnp.bfloat16)
    grad_upward = (grad_hidden * gate * sigma).astype(jnp.bfloat16)
    grad_ffn_part = (
        contract(grad_gate, wg_full, 1, 1) + contract(grad_upward, wu_full, 1, 1)
    ).astype(jnp.bfloat16)
    grad_ffn_part, grad_gate, grad_upward = tie(grad_ffn_part, grad_gate, grad_upward)
    grad_ffn_in = summed(grad_ffn_part)
    grad_wg = contract(ffn_rows, grad_gate, 0, 0).astype(jnp.bfloat16)
    grad_wu = contract(ffn_rows, grad_upward, 0, 0).astype(jnp.bfloat16)
    sum_ffn = ring.scatter([grad_wg, grad_wu])

    gain_part_ffn = jnp.sum(grad_ffn_in * middle * rate_ffn, axis=0)
    grad_middle = cot_rows.astype(jnp.float32) + norm_backward(
        grad_ffn_in, middle, rate_ffn, gain_ffn
    )
    branch_all = gathered((BRANCH * grad_middle).astype(jnp.bfloat16))
    branch_ffn, branch_all = tie(
        contract(hidden, full_down, 1, 1).astype(jnp.bfloat16), branch_all
    )
    out_rows = (middle + BRANCH * summed(branch_ffn)).astype(jnp.bfloat16)
    out_groups = exchange(packed(out_rows, back_order), -1)
    grad_mixed = contract(branch_all, wo_full, 1, 0).astype(jnp.bfloat16)
    grad_wo = contract(branch_all, attn_out, 0, 0).astype(jnp.bfloat16)
    sum_out = ring.scatter([grad_wo])
    grad_q, first, second, back = attend_back(
        qkv, prev, attn_out, grad_mixed, prob_one, prob_two, tables, tables_prev
    )
    back_route = [(i + 1, i) for i in range(rank_count - 1)]
    back, out_groups = tie(lax.ppermute(back, "wide", back_route), out_groups)
    second = (second + back.astype(jnp.float32)).astype(jnp.bfloat16)
    grad_k, grad_v = jnp.concatenate([first, second], axis=1)
    grad_wq = contract(attn_rows, grad_q, 0, 0).astype(jnp.bfloat16)
    grad_wk = contract(attn_rows, grad_k, 0, 0).astype(jnp.bfloat16)
    grad_wv = contract(attn_rows, grad_v, 0, 0).astype(jnp.bfloat16)
    sum_attn = ring.scatter([grad_wq, grad_wk, grad_wv])
    grad_attn_in = summed(
        contract(grad_q, wq_full, 1, 1)
        + contract(grad_k, wk_full, 1, 1)
        + contract(grad_v, wv_full, 1, 1)
    )
    gain_part_attn = jnp.sum(grad_attn_in * resid * rate_attn, axis=0)
    grad_resid = grad_middle + norm_backward(grad_attn_in, resid, rate_attn, gain_attn)
    grad_rows = (validity * grad_resid).astype(jnp.bfloat16)
    gains = total_over_all(jnp.stack([gain_part_attn, gain_part_ffn]))

    output = unpacked(out_groups, send_place)
    grad_tokens = unpacked(exchange(packed(grad_rows, back_order), -1), send_place)
    return (
        output,
        grad_tokens,
        gains[0],
        gains[1],
        sum_attn[0],
        sum_attn[1],
        sum_attn[2],
        sum_out[0].T,
        sum_ffn[0],
        sum_ffn[1],
        sum_down[0].T,
    )


def solution(mesh):
    rows = P(("wide", "narrow"), None)
    split_in = P("wide", "narrow")
    split_out = P("narrow", "wide")
    weights = (split_in, split_in, split_in, split_out, split_in, split_in, split_out)
    return jax.shard_map(
        body,
        mesh=mesh,
        in_specs=(rows, P(), P()) + weights + (rows, P(), P()),
        out_specs=(rows, rows, P(), P()) + weights,
        check_vma=False,
    )
```
